32 devices in a mesh: band: 8 (over z, y), ga: 4 (over x, core).
Axes of the slice: x: 2, y: 2, z: 4, core: 2. Of those that a mesh axis runs over, the one named last changes fastest.
Arguments:
- orbitals: float32 [8, 96, 9216], P('band', 'ga'), may hold values from -6 to 6
- retained: int32 [96, 9216], P(None, 'ga'), may hold values 0 or 1
Outputs:
- exchange_field: float32 [8, 96, 9216], P('band', 'ga')
- block_matrix: float32 [8, 1], P('band')
The draws below stay inside these ranges and needn't reach their ends.
All inputs are finite; a program needn't handle non-finite values. No bound on the sum of `retained` on one device may be relied on, other than what follows from the above.
Results may differ from the reference program's by a relative error of at most 0.0086.
Values may be sent and summed in bfloat16 or wider, within the bound.
A program may use at most 64 MiB of HBM per device.

```python
import jax
import jax.numpy as jnp
from jax import lax

N = 96
BD = 1
BANDS = 8
REACH = 1
N_BAND = 8


def place_ends(values, key, least, top_value):
    place = [jax.random.randint(jax.random.fold_in(key, axis), (), 0, length) for axis, length in enumerate(values.shape)]
    widest = values.shape.index(max(values.shape))
    beside = place[:widest] + [(place[widest] + 1) % values.shape[widest]] + place[widest + 1:]
    return values.at[tuple(place)].set(least).at[tuple(beside)].set(top_value)


def shard_levels(stream_key, extent, split, least, top_value):
    loudness = 1.0
    for dim, shards_of in split:
        steps = jax.random.uniform(jax.random.fold_in(jax.random.fold_in(stream_key, 6), dim), (shards_of,), jnp.float32, least / len(split), top_value / len(split))
        loudness = loudness * jnp.repeat(jnp.exp(steps), extent[dim] // shards_of).reshape((-1,) + (1,) * (len(extent) - 1 - dim))
    return loudness


def noise(key, extent, deviation, bound, split=(), kind=jnp.bfloat16):
    result = jax.random.normal(key, extent, jnp.float32) * deviation
    if len(split) > 0:
        result = shard_levels(key, extent, split, -0.22, 0.18) * result
    return jnp.clip(result, min=-bound, max=bound).astype(kind)


def setup_inputs(seed: int = 0) -> dict:
    key_list = jax.random.split(jax.random.key(seed), 3)
    return {
        "orbitals": noise(key_list[0], (BANDS, N, N * N), 1.0, 6.0, ((0, 8), (1, 4)), jnp.float32),
        "retained": place_ends((jax.random.randint(key_list[1], (N, N * N), 0, 4) < 3).astype(jnp.int32), jax.random.fold_in(key_list[1], 1), 0, 1),
    }


def cas_table(length):
    counter = jnp.arange(length, dtype=jnp.int32)
    product = counter[:, None] * counter[None, :] % length
    angles = 2.0 * jnp.pi / length * product.astype(jnp.float32)
    scaled = (jnp.cos(angles) + jnp.sin(angles)) / jnp.sqrt(jnp.float32(length))
    return scaled.astype(jnp.bfloat16)

def wrapped(indices, length):
    return jnp.where(indices < length // 2, indices, indices - length).astype(jnp.float32)

def screening(rows_x, rows_y, rows_z, length):
    freq_x = wrapped(rows_x, length)
    freq_y = wrapped(rows_y, length)
    freq_z = wrapped(rows_z, length)
    squared = freq_x[:, None, None] ** 2 + freq_y[None, :, None] ** 2 + freq_z[None, None, :] ** 2
    spread = length / 4.0
    return 1.0 / (1.0 + squared / (spread * spread))

def transform_axis(density, table, form):
    return jnp.einsum(form, density.astype(jnp.float32), table.astype(jnp.float32)).astype(jnp.bfloat16)

def potential(density, table, screen):
    sectioned = transform_axis(density, table, 'pxyz,kz->pxyk')
    sectioned = transform_axis(sectioned, table, 'pxyz,ky->pxkz')
    sectioned = transform_axis(sectioned, table, 'pxyz,kx->pkyz')
    sectioned = (sectioned.astype(jnp.float32) * screen).astype(jnp.bfloat16)
    sectioned = transform_axis(sectioned, table, 'pxyz,kx->pkyz')
    sectioned = transform_axis(sectioned, table, 'pxyz,ky->pxkz')
    return transform_axis(sectioned, table, 'pxyz,kz->pxyk')

def reference(orbitals, retained):
    lattice = orbitals.reshape(BANDS, N, N, N).astype(jnp.float32)
    table = cas_table(N)
    counter = jnp.arange(N, dtype=jnp.int32)
    screen = screening(counter, counter, counter, N) * retained.reshape(N, N, N).astype(jnp.float32)
    window = (2 * REACH + 1) * BD

    def one_block(block):
        offsets = jnp.arange(-REACH * BD, (REACH + 1) * BD, dtype=jnp.int32)
        indices = ((block * BD + offsets) % BANDS).astype(jnp.int32)
        visitors = lattice[indices]
        owned = lax.dynamic_slice_in_dim(lattice, (block * BD).astype(jnp.int32), BD, 0)
        density = (owned[:, None] * visitors[None]).astype(jnp.bfloat16).reshape(BD * window, N, N, N)
        fields = potential(density, table, screen).astype(jnp.float32).reshape(BD, window, N, N, N)
        running = lax.optimization_barrier(jnp.sum(fields * visitors[None], axis=1))
        intersection = jnp.dot(owned.reshape(BD, -1), running.reshape(BD, -1).T, precision=lax.Precision.HIGHEST) / float(N ** 3)
        return (running, intersection)
    fields_all, blocks_all = lax.map(one_block, jnp.arange(N_BAND, dtype=jnp.int32))
    return (fields_all.reshape(BANDS, N, N * N), blocks_all.reshape(BANDS, BD))
```

```python
import functools
import math

import jax
import jax.numpy as jnp
import numpy as np
from jax import lax
from jax.experimental import pallas as pl
from jax.experimental.pallas import tpu as pltpu
from jax.sharding import PartitionSpec as P

MESH = pl.DeviceIdType.MESH
LANES = 128


def cas_numpy(length):
    counter = np.arange(length)
    product = (counter[:, None] * counter[None, :] % length).astype(np.float32)
    angles = np.float32(2.0 * np.pi / length) * product
    return (np.cos(angles) + np.sin(angles)) / np.sqrt(np.float32(length))


def tables(length):
    pack = math.lcm(length, LANES) // length
    tiles = pack * length // LANES
    cas = cas_numpy(length)
    order = np.arange(length).reshape(length // pack, pack).T.reshape(-1)
    second = cas[order][:, order]
    spread = np.zeros((pack * LANES, pack * length), np.float32)
    for q in range(pack):
        spread[q * LANES : q * LANES + length, q * length : (q + 1) * length] = cas
    forward = np.stack(
        [spread[t * LANES : (t + 2) * LANES, t * LANES : (t + 1) * LANES] for t in range(tiles)]
    )
    backward = np.stack(
        [
            spread[0 : 2 * LANES, 0 : 2 * LANES].T,
            spread[2 * LANES : 4 * LANES, LANES : 3 * LANES].T,
        ]
    )
    as_bf16 = lambda v: jnp.asarray(v, jnp.bfloat16)
    return as_bf16(cas), as_bf16(second), as_bf16(forward), as_bf16(backward)


def wrapped_numpy(length):
    k = np.arange(length)
    return np.where(k < length // 2, k, k - length).astype(np.float32)


def split_lanes(tile_list):
    t0, t1, t2 = tile_list
    lane = lax.broadcasted_iota(jnp.int32, t0.shape, 1)
    roll = lambda v, s: pltpu.roll(v, s, 1)
    z1 = jnp.where(lane < 32, roll(t0, 32), roll(t1, 32))
    z2 = jnp.where(lane < 64, roll(t1, 64), roll(t2, 64))
    return [t0, z1, z2, roll(t2, 96)]


def join_lanes(z):
    lane = lax.broadcasted_iota(jnp.int32, z[0].shape, 1)
    roll = lambda v, s: pltpu.roll(v, s, 1)
    r1, r2, r3 = roll(z[1], 96), roll(z[2], 64), roll(z[3], 32)
    return [
        jnp.where(lane < 96, z[0], r1),
        jnp.where(lane < 64, r1, r2),
        jnp.where(lane < 32, r2, r3),
    ]


def dot(a, b):
    return jnp.dot(a, b, preferred_element_type=jnp.float32)


def exchange_kernel(
    length, groups, bands, give_back,
    phi_hbm, kept_hbm, plane_hbm, cas_hbm, second_hbm, fwd_hbm, bwd_hbm,
    out_ref, extra_ref,
    phi_ref, kept_ref, plane_ref, cas_ref, second_ref, fwd_ref, bwd_ref, own, guest, running, turn, screen, phi_out, phi_in,
    spec_out, spec_in, pot_out, pot_in, part_out, part_in, joined, sums, passed,
    load_sem, phi_sent, phi_got, fwd_sent, fwd_got, bwd_sent, bwd_got, part_sent, part_got, sum_sent, sum_got, pass_sent, pass_got,
):
    slab = length // groups
    pack = 4
    wide = pack * length
    blocks = length // pack
    dev_blocks = blocks // groups
    step = 8
    chunks = slab // step
    chunk_rows = blocks * step
    dev_rows = dev_blocks * step
    tiles = wide // LANES
    me = lax.axis_index("ga")
    band = lax.axis_index("band")
    upper = lax.rem(band + 1, bands)
    lower = lax.rem(band + bands - 1, bands)
    half = groups // 2
    chip, core = me // 2, me % 2
    offsets = [(dx, dc) for dx in range(half - 1, -1, -1) for dc in range(2) if (dx, dc) != (0, 0)]
    peers = [((chip + dx) % half) * 2 + (core + dc) % 2 for dx, dc in offsets]

    loads = [
        pltpu.make_async_copy(
            phi_hbm.at[pl.ds(c * step, step)], phi_ref.at[pl.ds(c * step, step)], load_sem.at[c]
        )
        for c in range(chunks)
    ]
    for src, dst in (
        (second_hbm, second_ref), (fwd_hbm, fwd_ref), (cas_hbm, cas_ref), (bwd_hbm, bwd_ref),
        (plane_hbm, plane_ref), (kept_hbm, kept_ref),
    ):
        loads.append(pltpu.make_async_copy(src, dst, load_sem.at[len(loads)]))
    for load in loads:
        load.start()
    barrier = pltpu.get_barrier_semaphore()
    for peer in peers:
        pl.semaphore_signal(barrier, inc=1, device_id=(band, peer), device_id_type=MESH)
    pl.semaphore_signal(barrier, inc=1, device_id=(lower, me), device_id_type=MESH)

    def send(src, dst, send_sem, recv_sem, target):
        copy = pltpu.make_async_remote_copy(
            src, dst, send_sem, recv_sem, device_id=target, device_id_type=MESH
        )
        copy.start()
        return copy

    def all_of(src, dst, send_sem, recv_sem):
        return pltpu.make_async_remote_copy(
            src, dst, send_sem, recv_sem, device_id=(upper, me), device_id_type=MESH
        )

    def split_tiles(value):
        return [value[:, t : t + LANES] for t in range(0, value.shape[1], LANES)]

    tiles_of = split_tiles

    def strided(c, i):
        return pl.ds(c * chunk_rows + i, blocks, stride=step)

    def planes(buf, c, i):
        return jnp.concatenate([turn[buf, q, strided(c, i), :] for q in range(pack)], axis=0)

    def put(buf, c, i, plane):
        for q in range(pack):
            turn[buf, q, strided(c, i), :] = plane[q * blocks : (q + 1) * blocks]

    def block_rows(c, b):
        return slice(c * chunk_rows + b * step, c * chunk_rows + (b + 2) * step)

    def unjoin(buf, c, b, both):
        for q, z in enumerate(split_lanes(tiles_of(both))):
            turn[buf, q, block_rows(c, b), :] = z

    def join(buf, c, b, target):
        found = join_lanes([turn[buf, q, block_rows(c, b), :] for q in range(pack)])
        for t, tile in enumerate(found):
            target[block_rows(c, b), t * LANES : (t + 1) * LANES] = tile.astype(target.dtype)

    def rows_of(ref, c):
        return ref.at[pl.ds(c * chunk_rows, chunk_rows)]

    phi_copies = []
    for c in range(chunks):
        loads[c].wait()
        for b in range(0, blocks, 2):
            both = jnp.concatenate(
                [
                    phi_ref[c * step : (c + 1) * step, (b + i) * wide : (b + i + 1) * wide]
                    for i in range(2)
                ],
                axis=0,
            )
            phi_out[block_rows(c, b), :] = both.astype(jnp.bfloat16)
            unjoin(0, c, b, both)
        if c == 0:
            pl.semaphore_wait(barrier, len(peers) + 1)
        phi_copies.append(
            send(rows_of(phi_out, c), rows_of(phi_in, c), phi_sent, phi_got.at[c], (upper, me))
        )
        for i in range(step):
            own[c * step + i] = planes(0, c, i)

    def forward(pair, c, left, right, buf):
        for i in range(0, step, 2):
            rho = jnp.concatenate(
                [
                    (left[c * step + i + j] * right[c * step + i + j]).astype(jnp.bfloat16)
                    for j in range(2)
                ],
                axis=1,
            )
            res = dot(second_ref[...], rho)
            for j in range(2):
                put(buf, c, i + j, res[:, j * LANES : (j + 1) * LANES])
        z = [
            turn[buf, q, c * chunk_rows : (c + 1) * chunk_rows, :].astype(jnp.bfloat16)
            for q in range(pack)
        ]
        for t in range(tiles):
            res = dot(jnp.concatenate([z[t], z[t + 1]], axis=1), fwd_ref[t]).astype(jnp.bfloat16)
            for g in range(groups):
                spec_out[pair, c, g, :, t * LANES : (t + 1) * LANES] = res[
                    g * dev_rows : (g + 1) * dev_rows
                ]
        for peer in peers:
            send(spec_out.at[pair, c, peer], spec_in.at[pair, c, me], fwd_sent, fwd_got.at[pair], (band, peer))
        spec_in[pair, c, me] = spec_out[pair, c, me]

    others = pl.ds(0, groups - 1)

    def middle(pair):
        arrived = spec_in.at[pair, :, others]
        all_of(arrived, arrived, fwd_sent, fwd_got.at[pair]).wait_recv()
        energy = jnp.zeros((step, LANES), jnp.float32)
        for b in range(0, dev_blocks, 2):
            lo, hi = b * step, (b + 2) * step
            parts = [
                spec_in[pair, c, s, lo:hi, :].astype(jnp.float32)
                for s in range(groups)
                for c in range(chunks)
            ]
            rhs = jnp.concatenate(
                [
                    jnp.concatenate([p[i * step : (i + 1) * step] for p in parts], axis=0)
                    for i in range(2)
                ],
                axis=1,
            ).astype(jnp.bfloat16)
            spectrum = dot(cas_ref[...], rhs)
            weighted = spectrum * screen[:, b * wide : (b + 2) * wide]
            for r in range(0, length, step):
                for tile in split_tiles(spectrum[r : r + step] * weighted[r : r + step]):
                    energy = energy + tile
            back = dot(cas_ref[...], weighted.astype(jnp.bfloat16))
            for s in range(groups):
                for c in range(chunks):
                    piece = back[s * slab + c * step : s * slab + (c + 1) * step]
                    pot_out[pair, c, s, lo:hi, :] = jnp.concatenate(
                        [piece[:, :wide], piece[:, wide:]], axis=0
                    ).astype(jnp.bfloat16)
        return energy

    def send_back(pair, c):
        for peer in peers:
            send(pot_out.at[pair, c, peer], pot_in.at[pair, c, me], bwd_sent, bwd_got.at[pair, c], (band, peer))
        pot_in[pair, c, me] = pot_out[pair, c, me]

    def backward(pair, c, buf, use):
        arrived = pot_in.at[pair, c, others]
        all_of(arrived, arrived, bwd_sent, bwd_got.at[pair, c]).wait_recv()
        value = pot_in[pair, c].reshape(chunk_rows, wide)
        for h in range(2):
            res = dot(value[:, h * LANES : (h + 2) * LANES], bwd_ref[h])
            for i in range(2):
                turn[buf, 2 * h + i, c * chunk_rows : (c + 1) * chunk_rows, :] = res[
                    :, i * LANES : (i + 1) * LANES
                ]
        for i in range(0, step, 2):
            two = jnp.concatenate([planes(buf, c, i), planes(buf, c, i + 1)], axis=1)
            res = dot(second_ref[...], two.astype(jnp.bfloat16))
            for j in range(2):
                use(c, i + j, res[:, j * LANES : (j + 1) * LANES])

    for load in loads[chunks : chunks + 4]:
        load.wait()
    for c in range(chunks):
        forward(0, c, own, own, 1)

    for load in loads[chunks + 4 :]:
        load.wait()
    freq = lax.broadcasted_iota(jnp.int32, (length, 1), 0)
    freq = jnp.where(freq < length // 2, freq, freq - length).astype(jnp.float32)
    scale = 1.0 / ((length / 4.0) * (length / 4.0))
    for c in range(0, dev_blocks):
        cols = slice(c * wide, (c + 1) * wide)
        squared = freq * freq + plane_ref[me, :, cols]
        screen[:, cols] = kept_ref[:, cols].astype(jnp.float32) / (1.0 + squared * scale)

    def guest_forward(c):
        phi_copies[c].wait_recv()
        for b in range(0, blocks, 2):
            unjoin(2, c, b, phi_in[block_rows(c, b), :].astype(jnp.float32))
        for i in range(step):
            guest[c * step + i] = planes(2, c, i)
        forward(1, c, own, guest, 1)

    def use_first(c, i, field):
        put(2, c, i, running[c * step + i] + field * own[c * step + i])

    def use_second(c, i, field):
        x = c * step + i
        put(1, c, i, field * own[x])
        running[x] = field * guest[x]

    for c in range(chunks):
        guest_forward(c)
    energy = middle(0)
    shared = middle(1)
    for c in range(chunks):
        send_back(1, c)
    if give_back:
        passed[0] = shared
        pass_copy = send(passed.at[0], passed.at[1], pass_sent, pass_got, (lower, me))
        sums[me] = energy + shared
    for c in range(chunks):
        send_back(0, c)
    part_copies = []
    for c in range(chunks):
        backward(1, c, 0, use_second)
        for b in range(0, blocks, 2):
            join(1, c, b, part_out)
        if give_back:
            part_copies.append(
                send(rows_of(part_out, c), rows_of(part_in, c), part_sent, part_got.at[c], (lower, me))
            )
    if give_back:
        pass_copy.wait_recv()
        sums[me] = sums[me] + passed[1]
        for peer in peers:
            send(sums.at[me], sums.at[me], sum_sent, sum_got, (band, peer))
    for c in range(chunks):
        backward(0, c, 0, use_first)
    for c in range(chunks):
        for b in range(0, blocks, 2):
            join(2, c, b, joined)
    if give_back:
        arrived = sums.at[others]
        all_of(arrived, arrived, sum_sent, sum_got).wait_recv()
        whole = sums[0]
        for s in range(1, groups):
            whole = whole + sums[s]
        whole = jnp.sum(jnp.sum(whole, axis=0, keepdims=True), axis=1, keepdims=True)
        extra_ref[...] = whole * (1.0 / float(length**3))
    else:
        extra_ref[...] = part_out[...]
    for c in range(chunks):
        if give_back:
            part_copies[c].wait_recv()
        for b in range(0, blocks, 2):
            value = joined[block_rows(c, b), :]
            if give_back:
                value = value + part_in[block_rows(c, b), :].astype(jnp.float32)
            for i in range(2):
                here = (0, slice(c * step, (c + 1) * step), slice((b + i) * wide, (b + i + 1) * wide))
                out_ref[here] = value[i * step : (i + 1) * step]
    all_of(phi_out, phi_in, phi_sent, phi_got.at[0]).wait_send()
    leaving = spec_out.at[:, :, others]
    all_of(leaving, leaving, fwd_sent, fwd_got.at[0]).wait_send()
    leaving = pot_out.at[:, :, others]
    all_of(leaving, leaving, bwd_sent, bwd_got.at[0, 0]).wait_send()
    if give_back:
        pass_copy.wait_send()
        leaving = sums.at[others]
        all_of(leaving, leaving, sum_sent, sum_got).wait_send()
        all_of(part_out, part_in, part_sent, part_got.at[0]).wait_send()


def fused(orbitals, retained, groups, bands, give_back):
    length = retained.shape[0]
    slab = length // groups
    pack = math.lcm(length, LANES) // length
    assert pack == 4 and orbitals.shape[0] == 1
    wide = pack * length
    blocks = length // pack
    rows = blocks * slab
    squares = wrapped_numpy(length) ** 2
    plane = (squares[:, None] + squares[None, :]).reshape(groups, 1, -1).astype(np.float32)
    plane = np.broadcast_to(plane, (groups, 1, plane.shape[2]))
    cas, second, fwd, bwd = tables(length)
    bf16, f32 = jnp.bfloat16, jnp.float32
    chunks = slab // 8
    exchange = lambda: pltpu.VMEM((2, chunks, groups, rows // groups // chunks, wide), bf16)
    merged = lambda kind: pltpu.VMEM((rows, wide), kind)
    cube = lambda: pltpu.VMEM((slab, length, LANES), f32)
    dma = pltpu.SemaphoreType.DMA
    extra = (
        jax.ShapeDtypeStruct((1, 1), f32) if give_back else jax.ShapeDtypeStruct((rows, wide), bf16)
    )
    vmem = pl.BlockSpec(memory_space=pltpu.VMEM)
    return pl.pallas_call(
        functools.partial(exchange_kernel, length, groups, bands, give_back),
        out_shape=(pltpu.VMEM((1, slab, length * length), f32), extra),
        in_specs=[pl.BlockSpec(memory_space=pltpu.HBM)] * 7,
        out_specs=(vmem, vmem),
        scratch_shapes=[
            pltpu.VMEM((slab, length * length), f32),
            pltpu.VMEM(retained.shape, jnp.int32),
            pltpu.VMEM(plane.shape, f32),
            *[pltpu.VMEM(v.shape, bf16) for v in (cas, second, fwd, bwd)],
            cube(), cube(), cube(),
            pltpu.VMEM((3, pack, rows, LANES), f32),
            pltpu.VMEM((length, length * length // groups), f32),
            merged(bf16), merged(bf16),
            exchange(), exchange(), exchange(), exchange(),
            merged(bf16), merged(bf16), merged(f32),
            pltpu.VMEM((groups, 8, LANES), f32), pltpu.VMEM((2, 8, LANES), f32),
            dma((chunks + 6,)), dma, dma((chunks,)),
            dma, dma((2,)), dma, dma((2, chunks)),
            *([dma, dma((chunks,)), dma, dma, dma, dma] if give_back else [dma] * 6),
        ],
        compiler_params=pltpu.CompilerParams(
            collective_id=0, has_side_effects=True, vmem_limit_bytes=62914560
        ),
    )(orbitals[0], retained, jnp.asarray(plane), cas, second, fwd, bwd)


def passed_along(value, axis, steps):
    count = lax.axis_size(axis)
    pairs = [(source, (source + steps) % count) for source in range(count)]
    return lax.ppermute(value, axis, pairs)


def transform_axis(density, table, form):
    return jnp.einsum(form, density, table, preferred_element_type=jnp.float32).astype(jnp.bfloat16)


def later_rounds(orbitals, retained, running, carried, band_reach):
    bands_dev, slab_rows, plane_cells = orbitals.shape
    length = retained.shape[0]
    groups = lax.axis_size("ga")
    column_rows = length // groups
    lattice = orbitals.reshape(bands_dev, slab_rows, length, length)
    table = jnp.asarray(cas_numpy(length), jnp.bfloat16)
    squares = jnp.asarray(wrapped_numpy(length) ** 2)
    local_y = lax.dynamic_slice_in_dim(squares, lax.axis_index("ga") * column_rows, column_rows)
    squared = squares[:, None, None] + local_y[None, :, None] + squares[None, None, :]
    spread = length / 4.0
    screen = retained.reshape(length, column_rows, length).astype(jnp.float32) / (
        1.0 + squared / (spread * spread)
    )

    def potentials(density):
        spectrum = transform_axis(density, table, "pxyz,kz->pxyk")
        spectrum = transform_axis(spectrum, table, "pxyz,ky->pxkz")
        spectrum = lax.all_to_all(spectrum, "ga", split_axis=2, concat_axis=1, tiled=True)
        spectrum = transform_axis(spectrum, table, "pxyz,kx->pkyz")
        spectrum = (spectrum.astype(jnp.float32) * screen).astype(jnp.bfloat16)
        spectrum = transform_axis(spectrum, table, "pxyz,kx->pkyz")
        spectrum = lax.all_to_all(spectrum, "ga", split_axis=1, concat_axis=2, tiled=True)
        spectrum = transform_axis(spectrum, table, "pxyz,ky->pxkz")
        return transform_axis(spectrum, table, "pxyz,kz->pxyk").astype(jnp.float32)

    def round_once(_, state):
        visiting, partial_field, running_sum = state
        visiting = passed_along(visiting, "band", 1)
        partial_field = passed_along(partial_field.astype(jnp.bfloat16), "band", 1)
        guests = visiting.astype(jnp.float32)
        fields = potentials((lattice * guests).astype(jnp.bfloat16))
        return (
            visiting,
            partial_field.astype(jnp.float32) + fields * lattice,
            running_sum + fields * guests,
        )

    visitors = passed_along(lattice.astype(jnp.bfloat16), "band", 1)
    _, carried, running = lax.fori_loop(
        1, band_reach, round_once,
        (visitors, carried.reshape(lattice.shape), running.reshape(lattice.shape)),
    )
    running = running + passed_along(
        carried.astype(jnp.bfloat16), "band", -band_reach
    ).astype(jnp.float32)
    flat, flat_running = lattice.reshape(bands_dev, -1), running.reshape(bands_dev, -1)
    block = jnp.dot(flat, flat_running.T, precision=lax.Precision.HIGHEST)
    return running.reshape(orbitals.shape), lax.psum(block, "ga") / float(length**3)


def local(orbitals, retained):
    groups, bands = lax.axis_size("ga"), lax.axis_size("band")
    band_reach = max(1, bands // 8)
    running, extra = fused(orbitals, retained, groups, bands, band_reach == 1)
    if band_reach == 1:
        return running, extra
    slab = orbitals.shape[1]
    wide = extra.shape[1]
    carried = extra.reshape(slab // 8, -1, 8, wide).transpose(0, 2, 1, 3).astype(jnp.float32)
    return later_rounds(orbitals, retained, running, carried.reshape(orbitals.shape), band_reach)


def solution(mesh):
    placed = (P("band", "ga", None), P(None, "ga"))
    return jax.shard_map(
        local,
        mesh=mesh,
        in_specs=placed,
        out_specs=(P("band", "ga", None), P("band", None)),
        check_vma=False,
    )
```
